128 devices in a mesh: row: 16 (over y, x), col: 8 (over z, core).
Axes of the slice: x: 4, y: 4, z: 4, core: 2. Of those that a mesh axis runs over, the one named last changes fastest.
Arguments:
- moments: float32 [2, 128, 128, 6144], P(None, None, 'row', 'col'), may hold values from -6 to 6
- owner_counts: int32 [16], replicated, may hold values from 1 to 16, 128 in all
Outputs:
- normalized: float32 [2, 32768, 6144], P(None, 'row', 'col')
- scales: float32 [2, 256], P(None, 'row')
- energy: float32 [2, 256], P(None, 'row')
The draws below stay inside these ranges and needn't reach their ends.
Inputs may be any that keep to these rules, and one draw needn't show every extreme that they name: owner_counts sums to 128, and its largest entry is exactly 16.
All inputs are finite; a program needn't handle non-finite values.
Results may differ from the reference program's by a relative error of at most 0.00002.
Values sent between devices are 32-bit elements.
No kernel may reach another device: no remote copies, remote signals or barrier semaphores. Data moves between devices by JAX's collectives and lax.ppermute only.
A program may use at most 128 MiB of HBM per device.

```python
import math
import jax
import jax.numpy as jnp
import numpy as np
from jax import lax

D = 6144
BLK = 128
TENSORS = 2
NB = 128
MOST = 16
N_ROW = 16


def level_of(rng, extent, cuts, smallest, largest):
    factor_of = 1.0
    for position, blocks in cuts:
        steps = jax.random.uniform(jax.random.fold_in(jax.random.fold_in(rng, 6), position), (blocks,), jnp.float32, smallest / len(cuts), largest / len(cuts))
        factor_of = factor_of * jnp.repeat(jnp.exp(steps), extent[position] // blocks).reshape((-1,) + (1,) * (len(extent) - 1 - position))
    return factor_of


def profile(amount, total, bound, skew):
    loads = [(1 << 20) // math.isqrt(standing ** skew) + 1 for standing in range(2, amount + 1)]
    surplus, given = total - bound - (amount - 1), [1] * (amount - 1)
    while surplus > 0:
        free = [i for i in range(amount - 1) if given[i] < bound]
        pool, budget = sum([loads[i] for i in free]), surplus
        for i in free:
            extra = min(bound - given[i], max(1, budget * loads[i] // pool), surplus)
            given[i] = given[i] + extra
            surplus = surplus - extra
    return np.array([bound] + given)


def ragged(stream_key, count, total, limit, lean):
    if count == 2:
        one = jax.random.randint(stream_key, (), max(1, total - limit), min(limit, total - 1) + 1)
        return jnp.stack([one, total - one])
    lengths = jnp.asarray(profile(count, total, limit, lean), jnp.int32)
    pairs = (count - 1) // 2
    donor, taker = lengths[1:1 + 2 * pairs:2], lengths[2:2 + 2 * pairs:2]
    margin = jnp.minimum(donor - 1, limit - taker)
    moved = jax.random.randint(jax.random.fold_in(stream_key, 1), (pairs,), 0, 1 << 20) % (margin + 1)
    lengths = lengths.at[1:1 + 2 * pairs:2].set(donor - moved).at[2:2 + 2 * pairs:2].set(taker + moved)
    return lengths[jax.random.permutation(jax.random.fold_in(stream_key, 2), count)]


def bell_draw(stream_key, dims, width, most, pieces=(), held_as=jnp.bfloat16):
    level = level_of(stream_key, dims, pieces, -0.22, 0.18) if pieces else 1.0
    drawn = jax.random.normal(stream_key, dims, jnp.float32) * width * level
    return jnp.minimum(jnp.maximum(drawn, -most), most).astype(held_as)


def setup_inputs(seed: int = 0) -> dict:
    key_of = jax.random.split(jax.random.key(seed), 3)
    return {
        "moments": bell_draw(key_of[0], (TENSORS, NB, BLK, D), 1.0, 6.0, ((2, 16), (3, 8)), jnp.float32),
        "owner_counts": ragged(key_of[1], N_ROW, NB, MOST, 2).astype(jnp.int32),
    }


def reference(moments, owner_counts):
    counts = owner_counts.astype(jnp.int32)
    starts = jnp.cumsum(counts) - counts
    slot_index = jnp.arange(MOST, dtype=jnp.int32)
    picked = starts[:, None] + slot_index[None, :]
    usable = slot_index[None, :] < counts[:, None]
    picked = jnp.where(usable, picked, 0).reshape(-1).astype(jnp.int32)
    usable_flat = usable.reshape(-1)

    def one_tensor(blocks):
        placed = jnp.where(usable_flat[:, None, None], jnp.take(blocks, picked, axis=0), jnp.zeros((), blocks.dtype))
        block_peak = jnp.max(jnp.abs(placed), axis=(1, 2))
        scale_value = jnp.maximum(block_peak, 1.0)
        scaled = (placed / scale_value[:, None, None]).reshape(-1, D)
        energy = jnp.sum(placed * placed, axis=(1, 2)) / (BLK * D)
        return scaled, scale_value, energy

    normalized, scales, energy = lax.map(one_tensor, moments)
    return normalized, scales, energy
```

```python
import functools

import jax
import jax.numpy as jnp
from jax import lax
from jax.experimental import pallas as pl
from jax.experimental.pallas import tpu as pltpu
from jax.sharding import PartitionSpec as P

CAP = 16


def stats_of(x):
    w = x.shape[-1]
    peak = jnp.abs(x[:, :, :128])
    total = x[:, :, :128] * x[:, :, :128]
    for c in range(128, w, 128):
        piece = x[:, :, c : c + 128]
        peak = jnp.maximum(peak, jnp.abs(piece))
        total = total + piece * piece
    peak = jnp.max(jnp.max(peak, axis=1), axis=1, keepdims=True)
    total = jnp.sum(jnp.sum(total, axis=1), axis=1, keepdims=True)
    return peak, total


def pack_kernel(counts, moments, packed, peak, total, held, sems):
    tensors, blocks = moments.shape[:2]
    groups = packed.shape[0]
    parts = sems.shape[1]
    step = blocks // parts
    copies = [
        [
            pltpu.make_async_copy(
                moments.at[t, pl.ds(p * step, step)],
                held.at[t, pl.ds(p * step, step)],
                sems.at[t, p],
            )
            for p in range(parts)
        ]
        for t in range(tensors)
    ]
    for t in range(tensors):
        for p in range(parts):
            copies[t][p].start()
    for t in range(tensors):
        for p in range(parts):
            copies[t][p].wait()

            def take_stats(i, _):
                at = pl.multiple_of(p * step + i * 8, 8)
                m, s = stats_of(held[t, pl.ds(at, 8)])
                peak[t, pl.ds(at, 8)] = m
                total[t, pl.ds(at, 8)] = s
                return 0

            lax.fori_loop(0, step // 8, take_stats, 0)

    def group(g, start):
        def slot(j, _):
            for t in range(tensors):
                packed[g, t, j] = held[t, start + j]
            return 0

        lax.fori_loop(0, counts[g], slot, 0)
        return start + counts[g]

    lax.fori_loop(0, groups, group, jnp.int32(0))


def place_kernel(info, inverse, arrived, out):
    t, j = pl.program_id(0), pl.program_id(1)
    sources, sub = arrived.shape[0], arrived.shape[3]

    @pl.when(j < info[0])
    def _():
        scale = inverse[t, j]
        for s in range(sources):
            out[0, s * sub : (s + 1) * sub, :] = arrived[s, t, j] * scale

    @pl.when(j >= info[0])
    def _():
        out[...] = jnp.zeros_like(out)


def on_device(moments, owner_counts):
    groups = lax.axis_size("row")
    splits = lax.axis_size("col")
    tensors, blocks, sub, width = moments.shape
    block_rows = sub * groups
    full_width = width * splits
    me = lax.axis_index("row")
    smem = pl.BlockSpec(memory_space=pltpu.SMEM)
    vmem = pl.BlockSpec(memory_space=pltpu.VMEM)
    parts = 4

    packed, peak, total = pl.pallas_call(
        pack_kernel,
        out_shape=(
            jax.ShapeDtypeStruct((groups, tensors, CAP, sub, width), jnp.float32),
            jax.ShapeDtypeStruct((tensors, blocks, 1), jnp.float32),
            jax.ShapeDtypeStruct((tensors, blocks, 1), jnp.float32),
        ),
        in_specs=[smem, pl.BlockSpec(memory_space=pl.ANY)],
        out_specs=(vmem, vmem, vmem),
        scratch_shapes=[
            pltpu.VMEM((tensors, blocks, sub, width), jnp.float32),
            pltpu.SemaphoreType.DMA((tensors, parts)),
        ],
        name="pack",
    )(owner_counts, moments)

    starts = jnp.cumsum(owner_counts) - owner_counts
    both = jnp.stack([peak[..., 0], total[..., 0]])
    both = lax.all_gather(both, "row")
    mine = jnp.minimum(starts[me] + jnp.arange(CAP), blocks - 1)
    both = jnp.stack([both[:, 0].max(0), both[:, 1].sum(0)])
    both = jnp.take(both, mine, axis=2)
    both = lax.all_gather(both, "col")
    used = jnp.arange(CAP) < owner_counts[me]
    block_peak = jnp.where(used, both[:, 0].max(0), 0.0)
    block_total = jnp.where(used, both[:, 1].sum(0), 0.0)
    scales = jnp.maximum(block_peak, 1.0)
    energy = block_total / (block_rows * full_width)

    arrived = lax.all_to_all(packed, "row", split_axis=0, concat_axis=0, tiled=True)
    normalized = pl.pallas_call(
        place_kernel,
        grid=(tensors, CAP),
        out_shape=jax.ShapeDtypeStruct((tensors, CAP * block_rows, width), jnp.float32),
        in_specs=[smem, smem, vmem],
        out_specs=pl.BlockSpec((1, block_rows, width), lambda t, j: (t, j, 0)),
        name="place",
    )(owner_counts[me][None], 1.0 / scales, arrived)
    return normalized, scales, energy


def solution(mesh):
    return jax.shard_map(
        on_device,
        mesh=mesh,
        in_specs=(P(None, None, "row", "col"), P()),
        out_specs=(P(None, "row", "col"), P(None, "row"), P(None, "row")),
        check_vma=False,
    )
```

```python
import functools

import jax
import jax.numpy as jnp
from jax import lax
from jax.experimental import pallas as pl
from jax.experimental.pallas import tpu as pltpu
from jax.sharding import PartitionSpec as P


SIDE = 4
GROUPS = SIDE * SIDE
HALF = 16
USUAL = 36
ALWAYS = SIDE * HALF
START, SPLIT, PLACE_A, PLACE_B, COUNT = (GROUPS * k for k in range(5))

SMEM = pl.BlockSpec(memory_space=pltpu.SMEM)
VMEM = pl.BlockSpec(memory_space=pltpu.VMEM)
HBM = pl.BlockSpec(memory_space=pl.ANY)


def in_vmem(x):
    return pltpu.with_memory_space_constraint(x, pltpu.VMEM)


def here():
    me = lax.axis_index("row")
    return lax.div(me, SIDE), lax.rem(me, SIDE)


def wrap(k):
    return lax.bitwise_and(k, SIDE - 1)


def shift(dy, dx):
    return [
        (g, (g // SIDE + dy) % SIDE * SIDE + (g % SIDE + dx) % SIDE) for g in range(GROUPS)
    ]


def stage_kernel(counts, moments, held, plan, need, column, row, sems):
    tensors = moments.shape[0]
    copies = [pltpu.make_async_copy(moments.at[t], held.at[t], sems.at[t]) for t in range(tensors)]
    for copy in copies:
        copy.start()

    start = jnp.int32(0)
    for k in range(SIDE):
        column[k] = jnp.int32(0)
        row[k] = jnp.int32(0)
    for g in range(GROUPS):
        count = counts[g]
        plan[COUNT + g] = count
        plan[START + g] = start
        plan[SPLIT + g] = count
        start = start + count
        column[g % SIDE] = column[g % SIDE] + count
        row[g // SIDE] = row[g // SIDE] + count

    def sweep(_, carry):
        for g in range(GROUPS):
            x, y = g % SIDE, g // SIDE
            items = 2 * plan[COUNT + g]
            split = plan[SPLIT + g]
            move = lax.shift_right_arithmetic(row[y] - column[x], 1)
            low = jnp.maximum(items - HALF, 0)
            high = jnp.minimum(items, HALF)
            changed = jnp.minimum(jnp.maximum(split + move, low), high)
            plan[SPLIT + g] = changed
            column[x] = column[x] + (changed - split)
            row[y] = row[y] - (changed - split)
        return carry

    lax.fori_loop(0, 3, sweep, 0)
    most = jnp.int32(0)
    for k in range(SIDE):
        most = jnp.maximum(most, jnp.maximum(column[k], row[k]))
        before = jnp.int32(0)
        for y in range(SIDE):
            plan[PLACE_A + y * SIDE + k] = before
            before = before + plan[SPLIT + y * SIDE + k]
        before = jnp.int32(0)
        for x in range(SIDE):
            g = k * SIDE + x
            plan[PLACE_B + g] = before
            before = before + 2 * plan[COUNT + g] - plan[SPLIT + g]
    need[0] = most
    for copy in copies:
        copy.wait()


def first_kernel(plan, held, *out):
    y, x = here()
    to_column, to_row, token = out[:SIDE], out[SIDE : 2 * SIDE], out[-1]
    token[...] = jnp.zeros_like(token)
    for d in range(SIDE):
        for k in range(SIDE):
            g = k * SIDE + wrap(x + d)
            start, place = plan[START + g], plan[PLACE_A + g]

            def put_a(i, carry, d=d, start=start, place=place):
                to_column[d][place + i] = held[
                    lax.bitwise_and(i, 1), start + lax.shift_right_logical(i, 1)
                ]
                return carry

            lax.fori_loop(0, plan[SPLIT + g], put_a, 0)
            g = wrap(y + d) * SIDE + k
            start, split, place = plan[START + g], plan[SPLIT + g], plan[PLACE_B + g] - plan[SPLIT + g]

            def put_b(i, carry, d=d, start=start, place=place):
                to_row[d][place + i] = held[
                    lax.bitwise_and(i, 1), start + lax.shift_right_logical(i, 1)
                ]
                return carry

            lax.fori_loop(split, 2 * plan[COUNT + g], put_b, 0)


def second_kernel(plan, token, *refs):
    y, x = here()
    from_column, from_row = refs[:SIDE], refs[SIDE : 2 * SIDE]
    to_owner_a, to_owner_b = refs[2 * SIDE : 3 * SIDE - 1], refs[3 * SIDE - 1 :]
    for d in range(1, SIDE):
        g = wrap(y + d) * SIDE + x
        place = plan[PLACE_A + g]

        def put_a(i, carry, d=d, place=place):
            for e in range(SIDE):
                to_owner_a[d - 1][e, i] = from_column[e][place + i]
            return carry

        lax.fori_loop(0, plan[SPLIT + g], put_a, 0)
        g = y * SIDE + wrap(x + d)
        place_b = plan[PLACE_B + g]

        def put_b(i, carry, d=d, place=place_b):
            for e in range(SIDE):
                to_owner_b[d - 1][e, i] = from_row[e][place + i]
            return carry

        lax.fori_loop(0, 2 * plan[COUNT + g] - plan[SPLIT + g], put_b, 0)


def place_kernel(plan, inverse, *refs):
    y, x = here()
    g = y * SIDE + x
    column, row = refs[:SIDE], refs[SIDE : 2 * SIDE]
    arrived_a = refs[2 * SIDE : 3 * SIDE - 1]
    arrived_b = refs[3 * SIDE - 1 : 4 * SIDE - 2]
    out, stage, sems = refs[4 * SIDE - 2 :]
    depth, block_rows = stage.shape[:2]
    sub = block_rows // GROUPS
    tensors = out.shape[0]
    count, split = plan[COUNT + g], plan[SPLIT + g]
    place_a, place_b = plan[PLACE_A + g], plan[PLACE_B + g]
    slots = out.shape[1] // block_rows * tensors

    def rows_of(dy, dx):
        source = wrap(y - dy) * SIDE + wrap(x - dx)
        return pl.ds(pl.multiple_of(source * sub, sub), sub)

    def write(i, at):
        t, j = lax.bitwise_and(i, 1), lax.shift_right_logical(i, 1)
        rows = pl.ds(pl.multiple_of(j * block_rows, block_rows), block_rows)
        return pltpu.make_async_copy(stage.at[at], out.at[t, rows], sems.at[at])

    def slot(i, carry):
        at = lax.rem(i, depth)

        @pl.when(i >= depth)
        def _():
            write(i - depth, at).wait()

        @pl.when(i < split)
        def _():
            scale = inverse[lax.bitwise_and(i, 1), lax.shift_right_logical(i, 1)]
            for dy in range(SIDE):
                for dx in range(SIDE):
                    piece = arrived_a[dy - 1][dx, i] if dy else column[dx][place_a + i]
                    stage[at, rows_of(dy, dx)] = piece * scale

        @pl.when((i >= split) & (i < 2 * count))
        def _():
            scale = inverse[lax.bitwise_and(i, 1), lax.shift_right_logical(i, 1)]
            k = i - split
            for dy in range(SIDE):
                for dx in range(SIDE):
                    piece = arrived_b[dx - 1][dy, k] if dx else row[dy][place_b + k]
                    stage[at, rows_of(dy, dx)] = piece * scale

        @pl.when(i >= 2 * count)
        def _():
            stage[at] = jnp.zeros_like(stage[at])

        write(i, at).start()
        return carry

    lax.fori_loop(0, slots, slot, 0)
    for i in range(slots - depth, slots):
        write(i, i % depth).wait()


def stats_kernel(token, held, out, peak, total):
    tensors, blocks, _, width = held.shape
    for t in range(tensors):

        def eight(i, carry, t=t):
            at = pl.multiple_of(i * 8, 8)
            x = held[t, pl.ds(at, 8)]
            high = jnp.abs(x[:, :, :128])
            square = x[:, :, :128] * x[:, :, :128]
            for c in range(128, width, 128):
                piece = x[:, :, c : c + 128]
                high = jnp.maximum(high, jnp.abs(piece))
                square = square + piece * piece
            peak[pl.ds(at, 8)] = jnp.max(high, axis=1)
            total[pl.ds(at, 8)] = jnp.sum(square, axis=1)
            return carry

        lax.fori_loop(0, blocks // 8, eight, 0)
        out[pl.ds(t, 1)] = jnp.max(peak[...].T, axis=0, keepdims=True)
        out[pl.ds(tensors + t, 1)] = jnp.sum(total[...].T, axis=0, keepdims=True)


def finish_kernel(plan, s0, s1, s2, s3, scales, energy, inverse, *, elements):
    y, x = here()
    g = y * SIDE + x
    start, count = plan[START + g], plan[COUNT + g]
    tensors, slots = scales.shape
    blocks = s0.shape[1]
    peak = jnp.maximum(jnp.maximum(s0[:tensors], s1[:tensors]), jnp.maximum(s2[:tensors], s3[:tensors]))
    total = (s0[tensors:] + s1[tensors:]) + (s2[tensors:] + s3[tensors:])
    both = jnp.concatenate([peak, total], axis=0)
    both = jnp.concatenate([both, jnp.zeros_like(both)], axis=0)
    both = pltpu.roll(both, lax.rem(blocks - start, blocks), 1)
    used = lax.broadcasted_iota(jnp.int32, both.shape, 1) < count
    both = jnp.where(used, both, 0.0)
    scale = jnp.maximum(both[:tensors, :slots], 1.0)
    scales[...] = scale
    inverse[...] = 1.0 / scale
    energy[...] = both[tensors : 2 * tensors, :slots] / elements


def joined(parts, tensors):
    high, total = parts[0][:tensors], parts[0][tensors:]
    for part in parts[1:]:
        high = jnp.maximum(high, part[:tensors])
        total = total + part[tensors:]
    return jnp.concatenate([high, total], axis=0)


def on_device(moments, owner_counts):
    splits = lax.axis_size("col")
    tensors, blocks, sub, width = moments.shape
    block_rows = sub * GROUPS
    slots = 2 * blocks // GROUPS
    params = lambda mib: pltpu.CompilerParams(vmem_limit_bytes=mib << 20)
    f32, i32 = jnp.float32, jnp.int32

    held, plan, need = pl.pallas_call(
        stage_kernel,
        out_shape=(
            pltpu.VMEM(moments.shape, f32),
            jax.ShapeDtypeStruct((5 * GROUPS,), i32),
            jax.ShapeDtypeStruct((1,), i32),
        ),
        in_specs=[SMEM, pl.BlockSpec(memory_space=pltpu.HBM)],
        out_specs=(VMEM, SMEM, SMEM),
        scratch_shapes=[
            pltpu.SMEM((SIDE,), i32),
            pltpu.SMEM((SIDE,), i32),
            pltpu.SemaphoreType.DMA((tensors,)),
        ],
        compiler_params=params(4),
        name="stage",
    )(owner_counts, pltpu.with_memory_space_constraint(moments, pltpu.HBM))

    def exchange(most, held, plan):
        lists = [pltpu.VMEM((most, sub, width), f32)] * (2 * SIDE)
        out = pl.pallas_call(
            first_kernel,
            out_shape=(*lists, jax.ShapeDtypeStruct((8, 128), f32)),
            in_specs=[SMEM, VMEM],
            out_specs=(VMEM,) * (2 * SIDE + 1),
            compiler_params=params(4),
            name="first",
        )(plan, in_vmem(held))
        to_column, to_row, token = out[:SIDE], out[SIDE : 2 * SIDE], out[-1]
        from_column = [to_column[0]] + [
            lax.ppermute(to_column[d], "row", shift(0, d)) for d in range(1, SIDE)
        ]
        from_row = [to_row[0]] + [
            lax.ppermute(to_row[d], "row", shift(d, 0)) for d in range(1, SIDE)
        ]

        stats = pl.pallas_call(
            stats_kernel,
            out_shape=jax.ShapeDtypeStruct((2 * tensors, blocks), f32),
            in_specs=[HBM, VMEM],
            out_specs=VMEM,
            scratch_shapes=[pltpu.VMEM((blocks, 128), f32)] * 2,
            compiler_params=params(4),
            name="stats",
        )(token, in_vmem(held))
        stats = joined(list(lax.all_gather(stats, "col")), tensors)
        stats = joined(
            [stats] + [lax.ppermute(stats, "row", shift(0, d)) for d in range(1, SIDE)], tensors
        )

        message = pltpu.VMEM((SIDE, HALF, sub, width), f32)
        out = pl.pallas_call(
            second_kernel,
            out_shape=(message,) * (2 * SIDE - 2),
            in_specs=[SMEM, HBM] + [VMEM] * (2 * SIDE),
            out_specs=(VMEM,) * (2 * SIDE - 2),
            compiler_params=params(4),
            name="second",
        )(plan, stats, *map(in_vmem, from_column + from_row))
        stats = [stats] + [lax.ppermute(stats, "row", shift(d, 0)) for d in range(1, SIDE)]
        arrived_a = [lax.ppermute(out[d - 1], "row", shift(d, 0)) for d in range(1, SIDE)]
        arrived_b = [
            lax.ppermute(out[SIDE - 1 + d - 1], "row", shift(0, d)) for d in range(1, SIDE)
        ]
        small = jax.ShapeDtypeStruct((tensors, slots), f32)
        scales, energy, inverse = pl.pallas_call(
            functools.partial(finish_kernel, elements=block_rows * width * splits),
            out_shape=(small,) * 3,
            in_specs=[SMEM] + [VMEM] * SIDE,
            out_specs=(VMEM,) * 3,
            compiler_params=params(4),
            name="finish",
        )(plan, *stats)
        depth = 4
        normalized = pl.pallas_call(
            place_kernel,
            out_shape=pltpu.HBM((tensors, slots * block_rows, width), f32),
            in_specs=[SMEM, SMEM] + [VMEM] * (4 * SIDE - 2),
            out_specs=HBM,
            scratch_shapes=[
                pltpu.VMEM((depth, block_rows, width), f32),
                pltpu.SemaphoreType.DMA((depth,)),
            ],
            compiler_params=params(4),
            name="place",
        )(plan, inverse, *map(in_vmem, from_column + from_row + arrived_a + arrived_b))
        return normalized, scales, energy

    return lax.cond(
        need[0] <= USUAL,
        functools.partial(exchange, USUAL),
        functools.partial(exchange, ALWAYS),
        held,
        plan,
    )


def solution(mesh):
    return jax.shard_map(
        on_device,
        mesh=mesh,
        in_specs=(P(None, None, "row", "col"), P()),
        out_specs=(P(None, "row", "col"), P(None, "row"), P(None, "row")),
        check_vma=False,
    )
```
